128 devices in a mesh: ya: 32 (over z, y, core), zb: 4 (over x).
Axes of the slice: x: 4, y: 4, z: 4, core: 2. Of those that a mesh axis runs over, the one named last changes fastest.
Arguments:
- source: float32 [512, 512, 512], P(None, 'ya', 'zb'), may hold values from -6 to 6
- symbol_x: float32 [512], replicated, may hold values from 0.3 to 3
- symbol_y: float32 [512], replicated, may hold values from 0.3 to 3
- symbol_z: float32 [512], replicated, may hold values from 0.3 to 3
Outputs:
- modes: float32 [512, 512, 512], P('ya', 'zb')
The draws below stay inside these ranges and needn't reach their ends.
All inputs are finite; a program needn't handle non-finite values.
Results may differ from the reference program's by a relative error of at most 0.000071.
Values sent between devices are 32-bit elements; how exact they have to be, the bound alone decides.
No kernel may reach another device: no remote copies, remote signals or barrier semaphores. Data moves between devices by JAX's collectives and lax.ppermute only.
A program may use at most 64 MiB of HBM per device.

```python
import jax
import jax.numpy as jnp
from jax import lax

GRID_X = 512
GRID_Y = 512
GRID_Z = 512


def block_levels(rng, shape, shards, low, top_value):
    def one(dim, parts):
        heights = jax.random.uniform(jax.random.fold_in(jax.random.fold_in(rng, 6), dim), (parts,), jnp.float32, low / len(shards), top_value / len(shards))
        return jnp.repeat(jnp.exp(heights), shape[dim] // parts).reshape((-1,) + (1,) * (len(shape) - dim - 1))

    gain = one(*shards[0])
    for cut in shards[1:]:
        gain = gain * one(*cut)
    return gain


def noise(rng, shape, width, limit, split=(), dtype=jnp.bfloat16):
    drawn = width * jax.random.normal(rng, shape, jnp.float32)
    if split:
        drawn = drawn * block_levels(rng, shape, split, -0.22, 0.18)
    return jnp.clip(drawn, -limit, limit).astype(dtype)


def setup_inputs(seed: int = 0) -> dict:
    splits = jax.random.split(jax.random.key(seed), 5)
    source = noise(splits[0], (GRID_X, GRID_Y, GRID_Z), 1.0, 6.0, ((1, 32), (2, 4)), jnp.float32)
    symbol_x = jnp.clip(jax.random.uniform(splits[1], (GRID_X,), jnp.float32, 0.3, 3.0), 0.3, 3.0)
    symbol_y = jnp.clip(jax.random.uniform(splits[2], (GRID_Y,), jnp.float32, 0.3, 3.0), 0.3, 3.0)
    symbol_z = jnp.clip(jax.random.uniform(splits[3], (GRID_Z,), jnp.float32, 0.3, 3.0), 0.3, 3.0)
    return {"source": source, "symbol_x": symbol_x, "symbol_y": symbol_y, "symbol_z": symbol_z}


def transform_table(count):
    rank = jnp.arange(count)
    angle = jnp.pi / (count + 1) * ((rank[:, None] + 1) * (rank[None, :] + 1) % (2 * count + 2)).astype(jnp.float32)
    return jnp.sin(angle) * (2.0 / (count + 1)) ** 0.5

def transform_dim(values, dim):
    moved = jnp.tensordot(values, transform_table(values.shape[dim]), axes=([dim], [0]), precision=lax.Precision.HIGHEST)
    return jnp.moveaxis(moved, -1, dim)

def reference(source, symbol_x, symbol_y, symbol_z):
    modes = source
    modes = transform_dim(modes, 0)
    modes = transform_dim(modes, 1)
    modes = transform_dim(modes, 2)
    symbol = symbol_x[:, None, None] + symbol_y[None, :, None] + symbol_z[None, None, :]
    modes = modes * lax.rsqrt(symbol)
    return modes
```

```python
import functools

import jax
import jax.numpy as jnp
import numpy as np
from jax import lax
from jax.experimental import pallas as pl
from jax.experimental.pallas import tpu as pltpu
from jax.sharding import PartitionSpec as P


N = 512
CHUNKS = (4, 6, 6)
STARTS = tuple(sum(CHUNKS[:k]) for k in range(len(CHUNKS)))
BF, F32 = jnp.bfloat16, jnp.float32
VM = pl.BlockSpec(memory_space=pltpu.VMEM)


def table():
    rank = np.arange(N)
    turns = (rank[:, None] + 1) * (rank[None, :] + 1) % (2 * N + 2)
    return (np.sin(np.pi / (N + 1) * turns) * np.sqrt(2.0 / (N + 1))).astype(np.float32)


def place(a):
    return a // 8, a // 2 % 4, a % 2


def index(z, y, core):
    return (z % 4 * 4 + y % 4) * 2 + core


def ring_pairs(stage, shift):
    pairs = []
    for a in range(32):
        z, y, core = place(a)
        along_z = core == stage
        pairs.append((a, index(z + shift * along_z, y + shift * (not along_z), core)))
    return pairs


def halves(value):
    high = value.astype(BF)
    return high, (value - high.astype(F32)).astype(BF)


def coords():
    a = lax.axis_index("ya")
    z, y, core = a // 8, a // 2 % 4, a % 2
    first = jnp.where(core == 0, z, y)
    second = jnp.where(core == 0, y, z)
    return first, second, core


def owner(first, second, core_axes, core):
    z = jnp.where(core_axes == 0, first, second)
    y = jnp.where(core_axes == 0, second, first)
    return (z * 4 + y) * 2 + core


def params(mib):
    return pltpu.CompilerParams(vmem_limit_bytes=mib * 2**20)


def x_kernel(sizes, src, tab, *refs):
    outs, rows = refs[:-1], refs[-1]
    first, second, core = coords()
    begin = 0
    for part, size in enumerate(sizes):
        skip = sum(sizes[:part])
        for rel in range(32):
            d1, d2, flip = rel // 8, rel // 2 % 4, rel % 2
            to = owner((first + d1) % 4, (second + d2) % 4, core, core ^ flip)
            rows[pl.ds(begin, size), :] = tab[to, skip : skip + size]
            begin += size
    high, low = halves(rows[...])
    left = jnp.concatenate([high, low, high], axis=1)
    for y in range(0, 16, 2):
        field = jnp.concatenate([src[pl.ds(y + i, N, stride=16), :] for i in range(2)], axis=1)
        high, low = halves(field)
        out = jnp.dot(left, jnp.concatenate([high, high, low]), preferred_element_type=F32)
        begin = 0
        for part, size in enumerate(sizes):
            for d1 in range(4):
                for i in range(2):
                    outs[part * 4 + d1][pl.ds(y + i, 8 * size, stride=16), :] = out[
                        begin : begin + 8 * size, i * 128 : (i + 1) * 128
                    ]
                begin += 8 * size


def x_transform(src, start, sizes):
    total = sum(sizes)
    tab = jnp.asarray(table().reshape(32, 16, N)[:, start : start + total])
    shapes = [jax.ShapeDtypeStruct((8 * size * 16, 128), F32) for size in sizes for _ in range(4)]
    return pl.pallas_call(
        functools.partial(x_kernel, sizes),
        out_shape=shapes,
        in_specs=[VM, VM],
        out_specs=[VM] * len(shapes),
        scratch_shapes=[pltpu.VMEM((total * 32, N), F32)],
        compiler_params=params(24),
        cost_estimate=pl.CostEstimate(
            flops=6 * total * 32 * N * 2048, bytes_accessed=2**22 + total * 2**18, transcendentals=0
        ),
        name="x_transform",
    )(src, tab)


def move(rows, *shapes):
    return dict(
        out_shape=[jax.ShapeDtypeStruct(shape, F32) for shape in shapes],
        out_specs=[VM] * len(shapes),
        compiler_params=params(8),
        cost_estimate=pl.CostEstimate(flops=rows * 4096, bytes_accessed=rows * 1024, transcendentals=0),
    )


def regroup_kernel(unit, b0, b1, b2, b3, *outs):
    for d, out in enumerate(outs, 1):
        for i, ref in enumerate((b0, b1, b2, b3)):
            out[i * 2 * unit : (i + 1) * 2 * unit, :] = ref[d * 2 * unit : (d + 1) * 2 * unit, :]


def regroup(size, blocks):
    unit = size * 16
    return pl.pallas_call(
        functools.partial(regroup_kernel, unit),
        in_specs=[VM] * 4,
        name="regroup",
        **move(24 * unit, *[(8 * unit, 128)] * 3),
    )(*blocks)


def gather_kernel(unit, b0, b1, b2, b3, c1, c2, c3, out):
    for i, ref in enumerate((b0, b1, b2, b3)):
        out[i * unit : (i + 1) * unit, :] = ref[unit : 2 * unit, :]
    for i, ref in enumerate((c1, c2, c3), 1):
        for d in range(4):
            at = (i * 4 + d) * unit
            out[at : at + unit, :] = ref[(2 * d + 1) * unit : (2 * d + 2) * unit, :]


def gather_other(size, own, moved):
    unit = size * 16
    return pl.pallas_call(
        functools.partial(gather_kernel, unit),
        in_specs=[VM] * 7,
        name="gather_other",
        **move(16 * unit, (16 * unit, 128)),
    )(*own, *moved)[0]


def y_kernel(size, tab, b0, b1, b2, b3, c1, c2, c3, other, *refs):
    outs, field = refs[:4], refs[4]
    first, second, core = coords()
    here = lax.axis_index("zb")
    left = jnp.concatenate(
        [tab[pl.ds(pl.multiple_of((here + d) % 4 * 128, 128), 128), :] for d in range(4)]
    )
    own = [b0, b1, b2, b3]
    moved = [None, c1, c2, c3]
    for j in range(0, size, 2):
        for d2 in range(4):
            for d1 in range(4):
                for mine in (True, False):
                    if mine:
                        at = owner((first + 4 - d1) % 4, (second + 4 - d2) % 4, core, core)
                        ref, block = (own[d1], 0) if d2 == 0 else (moved[d2], 2 * d1)
                    else:
                        at = owner((second + 4 - d1) % 4, (first + 4 - d2) % 4, core ^ 1, core ^ 1)
                        ref, block = other, d2 * 4 + d1
                    at = pl.multiple_of(at * 16, 16)
                    value = jnp.concatenate(
                        [ref[pl.ds((block * size + j + i) * 16, 16), :] for i in range(2)], axis=1
                    )
                    high, low = halves(value)
                    field[j // 2, 0, pl.ds(at, 16), :] = high
                    field[j // 2, 1, pl.ds(at, 16), :] = low
        high, low = field[j // 2, 0], field[j // 2, 1]
        out = jnp.dot(left, jnp.concatenate([high, high, low]), preferred_element_type=F32)
        for d in range(4):
            for i in range(2):
                outs[d][j + i] = out[d * 128 : (d + 1) * 128, i * 128 : (i + 1) * 128]


def y_transform(size, tab, own, moved, other):
    return pl.pallas_call(
        functools.partial(y_kernel, size),
        out_shape=[jax.ShapeDtypeStruct((size, 128, 128), F32)] * 4,
        in_specs=[VM] * 9,
        out_specs=[VM] * 4,
        scratch_shapes=[pltpu.VMEM((size // 2, 2, N, 256), BF)],
        compiler_params=params(16),
        cost_estimate=pl.CostEstimate(
            flops=6 * size * N * N * 128, bytes_accessed=2**20 + size * 2**19, transcendentals=0
        ),
        name="y_transform",
    )(tab, *own, *moved, other)


def z_kernel(start, size, tab, sx, sy, sz, d0, d1, d2, d3, *refs):
    out, result, sem = refs[-3:]
    here = lax.axis_index("zb")
    base = lax.axis_index("ya") * 16 + start
    right = jnp.concatenate(
        [
            tab[pl.ds(pl.multiple_of(part * N + (here + 4 - d) % 4 * 128, 128), 128), :]
            for part in (0, 1, 0)
            for d in range(4)
        ]
    )
    yz = jnp.concatenate([sy[...]] * 4, axis=1) + sz[...]
    copies = []
    for j in range(size):
        high, low = halves(jnp.concatenate([d[j] for d in (d0, d1, d2, d3)], axis=1))
        left = jnp.concatenate([high, high, low], axis=1)
        value = jnp.dot(left, right, preferred_element_type=F32)
        result[j] = value * lax.rsqrt(sx[base + j] + yz)
        copy = pltpu.make_async_copy(result.at[j], out.at[start + j], sem.at[j])
        copy.start()
        copies.append(copy)
    for copy in copies:
        copy.wait()


def z_transform(start, size, tab, sx, sy, sz, fields, into):
    more = [] if into is None else [into]
    return pl.pallas_call(
        functools.partial(z_kernel, start, size),
        out_shape=jax.ShapeDtypeStruct((16, 128, N), F32),
        in_specs=[VM, pl.BlockSpec(memory_space=pltpu.SMEM)]
        + [VM] * 6
        + [pl.BlockSpec(memory_space=pl.ANY)] * len(more),
        out_specs=pl.BlockSpec(memory_space=pl.ANY),
        scratch_shapes=[pltpu.VMEM((size, 128, N), F32), pltpu.SemaphoreType.DMA((size,))],
        input_output_aliases={8: 0} if more else {},
        compiler_params=params(16),
        cost_estimate=pl.CostEstimate(
            flops=6 * size * 128 * N * N, bytes_accessed=2**20 + size * 2**19, transcendentals=size * 128 * N
        ),
        name="z_transform",
    )(tab, sx, sy, sz, *fields, *more)


SHIFTS = (1, 3, 2)


def run(source, symbol_x, symbol_y, symbol_z):
    h = table()
    high = h.astype(jnp.bfloat16)
    low = (h - high.astype(np.float32)).astype(jnp.bfloat16)
    y_tab = jnp.asarray(np.concatenate([high, low, high], axis=1))
    z_tab = jnp.asarray(np.concatenate([high, low]))
    src = source.reshape(N * 16, 128)

    here = lax.axis_index("zb")
    sy = lax.dynamic_slice_in_dim(symbol_y, here * 128, 128)
    sy = jnp.broadcast_to(sy[:, None], (128, 128))
    sz = symbol_z[None, :]

    swap = [(a, a ^ 1) for a in range(32)]
    sent = list(x_transform(src, 0, CHUNKS[:1]))
    sent += list(x_transform(src, STARTS[1], CHUNKS[1:]))
    out = None
    for k, size in enumerate(CHUNKS):
        b = {0: sent[4 * k]}
        for d in SHIFTS:
            b[d] = lax.ppermute(sent[4 * k + d], "ya", ring_pairs(0, d))
        b = [b[d] for d in range(4)]
        groups = regroup(size, b)
        c = {}
        for d in SHIFTS:
            c[d] = lax.ppermute(groups[d - 1], "ya", ring_pairs(1, d))
        c = [c[d] for d in range(1, 4)]
        other = gather_other(size, b, c)
        other = lax.ppermute(other, "ya", swap)
        f = y_transform(size, y_tab, b, c, other)
        g = {0: f[0]}
        for d in SHIFTS:
            pairs = [(n, (n + d) % 4) for n in range(4)]
            g[d] = lax.ppermute(f[d], "zb", pairs)
        g = [g[d] for d in range(4)]
        out = z_transform(STARTS[k], size, z_tab, symbol_x, sy, sz, g, out)
    return out


def solution(mesh):
    placed = (P(None, "ya", "zb"), P(), P(), P())
    return jax.shard_map(
        run, mesh=mesh, in_specs=placed, out_specs=P("ya", "zb", None), check_vma=False
    )
```

```python
import functools
import math

import jax
import jax.numpy as jnp
import numpy as np
from jax import lax
from jax.experimental import pallas as pl
from jax.experimental.pallas import tpu as pltpu
from jax.sharding import PartitionSpec as P


N = 512
CHUNKS = (6, 4, 6)
MERGED = (1,)
STARTS = tuple(sum(CHUNKS[:k]) for k in range(len(CHUNKS)))
LEADS = tuple(sum(m < k for m in MERGED) % 2 for k in range(len(CHUNKS)))
BF, F32 = jnp.bfloat16, jnp.float32
VM = pl.BlockSpec(memory_space=pltpu.VMEM)


def table():
    rank = np.arange(N)
    turns = (rank[:, None] + 1) * (rank[None, :] + 1) % (2 * N + 2)
    return (np.sin(np.pi / (N + 1) * turns) * np.sqrt(2.0 / (N + 1))).astype(np.float32)


def place(a):
    return a // 8, a // 2 % 4, a % 2


def index(z, y, core):
    return (z % 4 * 4 + y % 4) * 2 + core


def ring_pairs(along, shift):
    pairs = []
    for a in range(32):
        z, y, core = place(a)
        in_z = core == along
        pairs.append((a, index(z + shift * in_z, y + shift * (not in_z), core)))
    return pairs


def halves(value):
    high = value.astype(BF)
    return high, (value - high.astype(F32)).astype(BF)


def coords(lead):
    a = lax.axis_index("ya")
    z, y, core = a // 8, a // 2 % 4, a % 2
    first = jnp.where(core == lead, z, y)
    second = jnp.where(core == lead, y, z)
    return first, second, core


def owner(lead, first, second, core_axes, core):
    z = jnp.where(core_axes == lead, first, second)
    y = jnp.where(core_axes == lead, second, first)
    return (z * 4 + y) * 2 + core


def params(mib):
    return pltpu.CompilerParams(vmem_limit_bytes=int(mib * 2**20))


def pair_of(rows):
    high, low = halves(rows)
    return high, jnp.concatenate([high, low])


def x_rows(size, lead, tab, rows):
    first, second, core = coords(lead)
    for rel in range(32):
        d1, d2, flip = rel // 8, rel // 2 % 4, rel % 2
        to = owner(lead, (first + d1) % 4, (second + d2) % 4, core, core ^ flip)
        rows[pl.ds(rel * size, size), :] = tab[to]
    return pair_of(rows[...])


def x_made_rows(size, lead, skip):
    first, second, core = coords(lead)
    shape = (32 * size, N)
    row = lax.broadcasted_iota(jnp.int32, shape, 0)
    rel = jnp.floor((row.astype(F32) + 0.5) * (1.0 / size)).astype(jnp.int32)
    one, two = (first + (rel >> 3)) & 3, (second + ((rel >> 1) & 3)) & 3
    swap = (core ^ lead).astype(jnp.int32)
    z, y = one + (two - one) * swap, two + (one - two) * swap
    mode = 16 * ((z * 4 + y) * 2 + (core ^ (rel & 1))) + skip + row - rel * size
    point = lax.broadcasted_iota(jnp.int32, shape, 1)
    turns = (mode + 1) * (point + 1)
    period = 2 * N + 2
    turns = turns - period * jnp.floor((turns.astype(F32) + 0.5) * (1.0 / period)).astype(jnp.int32)
    turns = turns.astype(F32)
    sign = jnp.where(turns > N + 1, -1.0, 1.0)
    turns = jnp.where(turns > N + 1, turns - (N + 1), turns)
    t = jnp.minimum(turns, N + 1 - turns) * np.float32(np.pi / (N + 1))
    square, series = t * t, 0.0
    for power in (13, 11, 9, 7, 5, 3):
        term = (-1) ** (power // 2) / math.factorial(power)
        series = (series + np.float32(term)) * square
    return pair_of((t + t * series) * (sign * np.float32(np.sqrt(2.0 / (N + 1)))))


def x_dot(size, left, high, low, y, outs):
    left_high, left_both = left
    both = jnp.dot(left_both, high, preferred_element_type=F32)
    out = both[: 32 * size] + (
        both[32 * size :] + jnp.dot(left_high, low, preferred_element_type=F32)
    )
    for d1 in range(4):
        for i in range(2):
            rows = out[d1 * 8 * size : (d1 + 1) * 8 * size, i * 128 : (i + 1) * 128]
            outs[d1][pl.ds(y + i, 8 * size, stride=16), :] = rows


def x_kernel(size, lead, field, tab, *refs):
    outs, rows = refs[:4], refs[4]
    left = x_rows(size, lead, tab, rows)
    for y in range(0, 16, 2):
        x_dot(size, left, field[y // 2, 0], field[y // 2, 1], y, outs)


def x_stream_kernel(size, lead, skip, src, *refs):
    outs, (field, parts, sem) = refs[:4], refs[4:]
    copies = []
    for i in range(2):
        copies.append(pltpu.make_async_copy(src.at[:, pl.ds(8 * i, 8), :], parts.at[i], sem.at[i]))
    for copy in copies:
        copy.start()
    left = x_made_rows(size, lead, skip)
    for i in range(2):
        copies[i].wait()
        flat = parts.at[i].reshape(N * 8, 128)
        for y in range(8 * i, 8 * i + 8, 2):
            pair = [flat[pl.ds(y - 8 * i + n, N, stride=8), :] for n in range(2)]
            high, low = halves(jnp.concatenate(pair, axis=1))
            field[y // 2, 0] = high
            field[y // 2, 1] = low
            x_dot(size, left, high, low, y, outs)


def x_transform(source, start, size, lead, stream):
    shapes = [jax.ShapeDtypeStruct((8 * size * 16, 128), F32)] * 4
    if stream:
        kernel = functools.partial(x_stream_kernel, size, lead, start)
        operands = [source]
        shapes = shapes + [jax.ShapeDtypeStruct((8, 2, N, 256), BF)]
        specs = [pl.BlockSpec(memory_space=pltpu.HBM)]
        scratch = [pltpu.VMEM((2, N, 8, 128), F32), pltpu.SemaphoreType.DMA((2,))]
    else:
        kernel = functools.partial(x_kernel, size, lead)
        operands = [source, jnp.asarray(table().reshape(32, 16, N)[:, start : start + size])]
        specs = [VM, VM]
        scratch = [pltpu.VMEM((size * 32, N), F32)]
    return pl.pallas_call(
        kernel,
        out_shape=shapes,
        in_specs=specs,
        out_specs=[VM] * len(shapes),
        scratch_shapes=scratch,
        compiler_params=params(46.5 if stream else 14),
        cost_estimate=pl.CostEstimate(
            flops=6 * size * 32 * N * 2048, bytes_accessed=2**22 + size * 2**18, transcendentals=0
        ),
        name="x_transform",
    )(*operands)


def move(rows, *shapes):
    return dict(
        out_shape=[jax.ShapeDtypeStruct(shape, F32) for shape in shapes],
        out_specs=[VM] * len(shapes),
        compiler_params=params(2),
        cost_estimate=pl.CostEstimate(flops=rows * 4096, bytes_accessed=rows * 1024, transcendentals=0),
    )


def regroup_kernel(unit, skip, more, *refs):
    blocks, after, outs = refs[:4], refs[4:-4], refs[-4:]
    for d, out in enumerate(outs):
        for i, ref in enumerate(blocks):
            at = d * 2 * unit + (skip if i else 0)
            out[i * 2 * unit : (i + 1) * 2 * unit, :] = ref[at : at + 2 * unit, :]
        if more and d:
            out[8 * unit :, :] = after[d - 1][...]


def regroup(size, skip, blocks, after):
    unit = size * 16
    more = after[0].shape[0] if after else 0
    shapes = [(8 * unit, 128)] + [(8 * unit + more, 128)] * 3
    return pl.pallas_call(
        functools.partial(regroup_kernel, unit, skip, more),
        in_specs=[VM] * (4 + len(after)),
        name="regroup",
        **move(32 * unit + 3 * more, *shapes),
    )(*blocks, *after)


def gather_kernel(unit, *refs):
    out = refs[4]
    for i, ref in enumerate(refs[:4]):
        for d in range(4):
            at = (i * 4 + d) * unit
            out[at : at + unit, :] = ref[(2 * d + 1) * unit : (2 * d + 2) * unit, :]


def gather_other(size, blocks):
    unit = size * 16
    return pl.pallas_call(
        functools.partial(gather_kernel, unit),
        in_specs=[VM] * 4,
        name="gather_other",
        **move(16 * unit, (16 * unit, 128)),
    )(*blocks)[0]


def y_kernel(size, lead, tab, c0, c1, c2, c3, other, *refs):
    outs, field = refs[:4], refs[4]
    first, second, core = coords(lead)
    here = lax.axis_index("zb")
    left = jnp.concatenate(
        [tab[pl.ds(pl.multiple_of((here + d) % 4 * 128, 128), 128), :] for d in range(4)]
    )
    for d2, ref in enumerate((c0, c1, c2, c3)):
        for d1 in range(4):
            for mine in (True, False):
                if mine:
                    at = owner(lead, (first + 4 - d1) % 4, (second + 4 - d2) % 4, core, core)
                    source, block = ref, 2 * d1
                else:
                    at = owner(lead, (second + 4 - d1) % 4, (first + 4 - d2) % 4, core ^ 1, core ^ 1)
                    source, block = other, d2 * 4 + d1
                at = pl.multiple_of(at * 16, 16)
                value = jnp.concatenate(
                    [source[pl.ds((block * size + j) * 16, 16), :] for j in range(size)], axis=1
                )
                high, low = halves(value)
                field[0, pl.ds(at, 16), :] = high
                field[1, pl.ds(at, 16), :] = low
    high, low = field[0], field[1]
    out = jnp.dot(left, jnp.concatenate([high, high, low]), preferred_element_type=F32)
    for d in range(4):
        for j in range(size):
            outs[d][j] = out[d * 128 : (d + 1) * 128, j * 128 : (j + 1) * 128]


def y_transform(size, lead, tab, blocks, other):
    return pl.pallas_call(
        functools.partial(y_kernel, size, lead),
        out_shape=[jax.ShapeDtypeStruct((size, 128, 128), F32)] * 4,
        in_specs=[VM] * 6,
        out_specs=[VM] * 4,
        scratch_shapes=[pltpu.VMEM((2, N, size * 128), BF)],
        compiler_params=params(12),
        cost_estimate=pl.CostEstimate(
            flops=6 * size * N * N * 128, bytes_accessed=2**20 + size * 2**19, transcendentals=0
        ),
        name="y_transform",
    )(tab, *blocks, other)


def z_right(tab, shifts):
    here = lax.axis_index("zb")
    order = [(here + 4 - d) % 4 * 128 for d in shifts]
    return jnp.concatenate(
        [tab[pl.ds(pl.multiple_of(part * N + o, 128), 128), :] for part in (0, 1, 0) for o in order]
    )


def z_dot(fields, rows, right):
    field = jnp.concatenate([jnp.concatenate([f[j] for f in fields], axis=1) for j in rows])
    high, low = halves(field)
    left = jnp.concatenate([high, high, low], axis=1)
    return jnp.dot(left, right, preferred_element_type=F32)


def z_part_kernel(size, shifts, tab, *refs):
    fields, out = refs[:-1], refs[-1]
    right = z_right(tab, shifts)
    for rows in (range(size // 2), range(size // 2, size)):
        value = z_dot(fields, rows, right)
        for i, j in enumerate(rows):
            out[j] = value[i * 128 : (i + 1) * 128]


def z_part(size, shifts, tab, fields):
    return pl.pallas_call(
        functools.partial(z_part_kernel, size, shifts),
        out_shape=jax.ShapeDtypeStruct((size, 128, N), F32),
        in_specs=[VM] * (1 + len(fields)),
        out_specs=VM,
        compiler_params=params(12),
        cost_estimate=pl.CostEstimate(
            flops=3 * size * 128 * N * N, bytes_accessed=2**20 + size * 2**19, transcendentals=0
        ),
        name="z_part",
    )(tab, *fields)


def z_kernel(start, size, shifts, partial, pieces, tab, sx, sy, sz, *refs):
    out, result, sem = refs[-3:]
    fields = refs[: len(shifts)]
    before = refs[len(shifts)] if partial else None
    here = lax.axis_index("zb")
    base = lax.axis_index("ya") * 16 + start
    right = z_right(tab, shifts)
    along = jnp.broadcast_to(sy[:, pl.ds(pl.multiple_of(here * 128, 128), 128)], (128, 128)).T
    yz = jnp.concatenate([along] * 4, axis=1) + sz[...]
    copies = []
    cuts = [size * n // pieces for n in range(pieces + 1)]
    for begin, end in zip(cuts, cuts[1:]):
        value = z_dot(fields, range(begin, end), right)
        for j in range(begin, end):
            part = value[(j - begin) * 128 : (j - begin + 1) * 128]
            if partial:
                part = part + before[j]
            result[j] = part * lax.rsqrt(sx[base + j] + yz)
            copy = pltpu.make_async_copy(result.at[j], out.at[start + j], sem.at[j])
            copy.start()
            copies.append(copy)
    for copy in copies:
        copy.wait()


def z_transform(start, size, shifts, tab, sx, sy, sz, fields, before, into):
    more = [] if into is None else [into]
    done = [] if before is None else [before]
    count = len(fields) + len(done)
    return pl.pallas_call(
        functools.partial(z_kernel, start, size, shifts, bool(done), 3 if done else 2),
        out_shape=jax.ShapeDtypeStruct((16, 128, N), F32),
        in_specs=[VM, pl.BlockSpec(memory_space=pltpu.SMEM)]
        + [VM] * (2 + count)
        + [pl.BlockSpec(memory_space=pltpu.HBM)] * len(more),
        out_specs=pl.BlockSpec(memory_space=pltpu.HBM),
        scratch_shapes=[pltpu.VMEM((size, 128, N), F32), pltpu.SemaphoreType.DMA((size,))],
        input_output_aliases={4 + count: 0} if more else {},
        compiler_params=params(12),
        cost_estimate=pl.CostEstimate(
            flops=6 * size * 128 * N * N, bytes_accessed=2**20 + size * 2**19, transcendentals=size * 128 * N
        ),
        name="z_transform",
    )(tab, sx, sy, sz, *fields, *done, *more)


SHIFTS = (1, 3, 2)


def run(source, symbol_x, symbol_y, symbol_z):
    h = table()
    high = h.astype(jnp.bfloat16)
    low = (h - high.astype(np.float32)).astype(jnp.bfloat16)
    y_tab = jnp.asarray(np.concatenate([high, low, high], axis=1))
    z_tab = jnp.asarray(np.concatenate([high, low]))

    sy, sz = symbol_y[None, :], symbol_z[None, :]

    swap = [(a, a ^ 1) for a in range(32)]
    made = []
    for k, size in enumerate(CHUNKS):
        outs = x_transform(source if k == 0 else field, STARTS[k], size, LEADS[k], k == 0)
        made.append(outs[:4])
        field = outs[4] if k == 0 else field
    out, arrived = None, None
    for k, size in enumerate(CHUNKS):
        if arrived is None:
            b, skip = {}, 0
            for d in SHIFTS:
                b[d] = lax.ppermute(made[k][d], "ya", ring_pairs(LEADS[k], d))
        else:
            b, skip = arrived, CHUNKS[k - 1] * 128
        merge = k in MERGED
        after = made[k + 1][1:] if merge else []
        groups = regroup(size, skip, [made[k][0], b[1], b[2], b[3]], after)
        c = {}
        for d in SHIFTS:
            c[d] = lax.ppermute(groups[d], "ya", ring_pairs(1 - LEADS[k], d))
        arrived = c if merge else None
        c = [groups[0], c[1], c[2], c[3]]
        other = gather_other(size, c)
        other = lax.ppermute(other, "ya", swap)
        f = y_transform(size, LEADS[k], y_tab, c, other)
        g = {0: f[0]}
        for d in SHIFTS:
            pairs = [(n, (n + d) % 4) for n in range(4)]
            g[d] = lax.ppermute(f[d], "zb", pairs)
        shifts, before = (0, *SHIFTS), None
        if k == len(CHUNKS) - 1:
            shifts, early = shifts[3:], shifts[:3]
            before = z_part(size, early, z_tab, [g[d] for d in early])
        fields = [g[d] for d in shifts]
        out = z_transform(STARTS[k], size, shifts, z_tab, symbol_x, sy, sz, fields, before, out)
    return out


def solution(mesh):
    placed = (P(None, "ya", "zb"), P(), P(), P())
    return jax.shard_map(
        run, mesh=mesh, in_specs=placed, out_specs=P("ya", "zb", None), check_vma=False
    )
```

```python
import functools
import math

import jax
import jax.numpy as jnp
import numpy as np
from jax import lax
from jax.experimental import pallas as pl
from jax.experimental.pallas import tpu as pltpu
from jax.sharding import PartitionSpec as P


N = 512
CHUNKS = (4, 4, 4, 4)
MERGED = (1,)
STARTS = tuple(sum(CHUNKS[:k]) for k in range(len(CHUNKS)))
LEADS = tuple(sum(m < k for m in MERGED) % 2 for k in range(len(CHUNKS)))
BF, F32 = jnp.bfloat16, jnp.float32
VM = pl.BlockSpec(memory_space=pltpu.VMEM)


def table():
    rank = np.arange(N)
    turns = (rank[:, None] + 1) * (rank[None, :] + 1) % (2 * N + 2)
    return (np.sin(np.pi / (N + 1) * turns) * np.sqrt(2.0 / (N + 1))).astype(np.float32)


def place(a):
    return a // 8, a // 2 % 4, a % 2


def index(z, y, core):
    return (z % 4 * 4 + y % 4) * 2 + core


def ring_pairs(along, shift):
    pairs = []
    for a in range(32):
        z, y, core = place(a)
        in_z = core == along
        pairs.append((a, index(z + shift * in_z, y + shift * (not in_z), core)))
    return pairs


def halves(value):
    high = value.astype(BF)
    return high, (value - high.astype(F32)).astype(BF)


def coords(lead):
    a = lax.axis_index("ya")
    z, y, core = a // 8, a // 2 % 4, a % 2
    first = jnp.where(core == lead, z, y)
    second = jnp.where(core == lead, y, z)
    return first, second, core


def owner(lead, first, second, core_axes, core):
    z = jnp.where(core_axes == lead, first, second)
    y = jnp.where(core_axes == lead, second, first)
    return (z * 4 + y) * 2 + core


def params(mib):
    return pltpu.CompilerParams(vmem_limit_bytes=int(mib * 2**20))


def pair_of(rows):
    high, low = halves(rows)
    return high, jnp.concatenate([high, low])


def x_rows(size, lead, tab, rows):
    first, second, core = coords(lead)
    for rel in range(32):
        d1, d2, flip = rel // 8, rel // 2 % 4, rel % 2
        to = owner(lead, (first + d1) % 4, (second + d2) % 4, core, core ^ flip)
        rows[pl.ds(rel * size, size), :] = tab[to]
    return pair_of(rows[...])


def x_made_rows(size, lead, skip):
    first, second, core = coords(lead)
    shape = (32 * size, N)
    row = lax.broadcasted_iota(jnp.int32, shape, 0)
    rel = jnp.floor((row.astype(F32) + 0.5) * (1.0 / size)).astype(jnp.int32)
    one, two = (first + (rel >> 3)) & 3, (second + ((rel >> 1) & 3)) & 3
    swap = (core ^ lead).astype(jnp.int32)
    z, y = one + (two - one) * swap, two + (one - two) * swap
    mode = 16 * ((z * 4 + y) * 2 + (core ^ (rel & 1))) + skip + row - rel * size
    point = lax.broadcasted_iota(jnp.int32, shape, 1)
    turns = (mode + 1) * (point + 1)
    period = 2 * N + 2
    turns = turns - period * jnp.floor((turns.astype(F32) + 0.5) * (1.0 / period)).astype(jnp.int32)
    turns = turns.astype(F32)
    sign = jnp.where(turns > N + 1, -1.0, 1.0)
    turns = jnp.where(turns > N + 1, turns - (N + 1), turns)
    t = jnp.minimum(turns, N + 1 - turns) * np.float32(np.pi / (N + 1))
    square, series = t * t, 0.0
    for power in (13, 11, 9, 7, 5, 3):
        term = (-1) ** (power // 2) / math.factorial(power)
        series = (series + np.float32(term)) * square
    return pair_of((t + t * series) * (sign * np.float32(np.sqrt(2.0 / (N + 1)))))


def x_dot(size, left, high, low, y, outs):
    left_high, left_both = left
    both = jnp.dot(left_both, high, preferred_element_type=F32)
    out = both[: 32 * size] + (
        both[32 * size :] + jnp.dot(left_high, low, preferred_element_type=F32)
    )
    for d1 in range(4):
        for i in range(2):
            rows = out[d1 * 8 * size : (d1 + 1) * 8 * size, i * 128 : (i + 1) * 128]
            outs[d1][pl.ds(y + i, 8 * size, stride=16), :] = rows


def x_kernel(size, lead, field, tab, *refs):
    outs, rows = refs[:4], refs[4]
    left = x_rows(size, lead, tab, rows)
    for y in range(0, 16, 2):
        x_dot(size, left, field[y // 2, 0], field[y // 2, 1], y, outs)


def x_stream_kernel(size, lead, skip, src, *refs):
    outs, (field, parts, sem) = refs[:4], refs[4:]
    copies = []
    for i in range(2):
        copies.append(pltpu.make_async_copy(src.at[:, pl.ds(8 * i, 8), :], parts.at[i], sem.at[i]))
    for copy in copies:
        copy.start()
    left = x_made_rows(size, lead, skip)
    for i in range(2):
        copies[i].wait()
        flat = parts.at[i].reshape(N * 8, 128)
        for y in range(8 * i, 8 * i + 8, 2):
            pair = [flat[pl.ds(y - 8 * i + n, N, stride=8), :] for n in range(2)]
            high, low = halves(jnp.concatenate(pair, axis=1))
            field[y // 2, 0] = high
            field[y // 2, 1] = low
            x_dot(size, left, high, low, y, outs)


def x_transform(source, start, size, lead, stream):
    shapes = [jax.ShapeDtypeStruct((8 * size * 16, 128), F32)] * 4
    if stream:
        kernel = functools.partial(x_stream_kernel, size, lead, start)
        operands = [source]
        shapes = shapes + [jax.ShapeDtypeStruct((8, 2, N, 256), BF)]
        specs = [pl.BlockSpec(memory_space=pltpu.HBM)]
        scratch = [pltpu.VMEM((2, N, 8, 128), F32), pltpu.SemaphoreType.DMA((2,))]
    else:
        kernel = functools.partial(x_kernel, size, lead)
        operands = [source, jnp.asarray(table().reshape(32, 16, N)[:, start : start + size])]
        specs = [VM, VM]
        scratch = [pltpu.VMEM((size * 32, N), F32)]
    return pl.pallas_call(
        kernel,
        out_shape=shapes,
        in_specs=specs,
        out_specs=[VM] * len(shapes),
        scratch_shapes=scratch,
        compiler_params=params(47.2 if stream else 14),
        cost_estimate=pl.CostEstimate(
            flops=6 * size * 32 * N * 2048, bytes_accessed=2**22 + size * 2**18, transcendentals=0
        ),
        name="x_transform",
    )(*operands)


def move(rows, *shapes):
    return dict(
        out_shape=[jax.ShapeDtypeStruct(shape, F32) for shape in shapes],
        out_specs=[VM] * len(shapes),
        compiler_params=params(2),
        cost_estimate=pl.CostEstimate(flops=rows * 4096, bytes_accessed=rows * 1024, transcendentals=0),
    )


def regroup_kernel(unit, skip, more, *refs):
    blocks, after, outs = refs[:4], refs[4:-4], refs[-4:]
    for d, out in enumerate(outs):
        for i, ref in enumerate(blocks):
            at = d * 2 * unit + (skip if i else 0)
            out[i * 2 * unit : (i + 1) * 2 * unit, :] = ref[at : at + 2 * unit, :]
        if more and d:
            out[8 * unit :, :] = after[d - 1][...]


def regroup(size, skip, blocks, after):
    unit = size * 16
    more = after[0].shape[0] if after else 0
    shapes = [(8 * unit, 128)] + [(8 * unit + more, 128)] * 3
    return pl.pallas_call(
        functools.partial(regroup_kernel, unit, skip, more),
        in_specs=[VM] * (4 + len(after)),
        name="regroup",
        **move(32 * unit + 3 * more, *shapes),
    )(*blocks, *after)


def gather_kernel(unit, *refs):
    out = refs[4]
    for i, ref in enumerate(refs[:4]):
        for d in range(4):
            at = (i * 4 + d) * unit
            out[at : at + unit, :] = ref[(2 * d + 1) * unit : (2 * d + 2) * unit, :]


def gather_other(size, blocks):
    unit = size * 16
    return pl.pallas_call(
        functools.partial(gather_kernel, unit),
        in_specs=[VM] * 4,
        name="gather_other",
        **move(16 * unit, (16 * unit, 128)),
    )(*blocks)[0]


def y_kernel(size, lead, sides, tab, *refs):
    field = refs[-1]
    first, second, core = coords(lead)
    here = lax.axis_index("zb")
    columns = [part * N + (core ^ side) * 256 for part in (0, 1, 0) for side in sides]
    left = [
        jnp.concatenate([tab[pl.ds(pl.multiple_of((here + d) % 4 * 128, 128), 128),
                             pl.ds(pl.multiple_of(c, 128), 256)] for d in range(4)])
        for c in columns
    ]
    left = jnp.concatenate(left, axis=1)
    for n, side in enumerate(sides):
        for d2 in range(4):
            for d1 in range(4):
                if side == 0:
                    at = owner(lead, (first + 4 - d1) % 4, (second + 4 - d2) % 4, core, 0)
                    source, block = refs[d2], 2 * d1
                else:
                    at = owner(lead, (second + 4 - d1) % 4, (first + 4 - d2) % 4, core ^ 1, 0)
                    source, block = refs[4 if 0 in sides else 0], d2 * 4 + d1
                at = pl.multiple_of(n * 256 + at * 8, 16)
                value = jnp.concatenate(
                    [source[pl.ds((block * size + j) * 16, 16), :] for j in range(size)], axis=1
                )
                high, low = halves(value)
                field[0, pl.ds(at, 16), :] = high
                field[1, pl.ds(at, 16), :] = low
    high, low = field[0], field[1]
    out = jnp.dot(left, jnp.concatenate([high, high, low]), preferred_element_type=F32)
    if 1 not in sides:
        refs[4][...] = out
        return
    if 0 not in sides:
        out = out + refs[1][...]
    outs = refs[-5:-1]
    for d in range(4):
        for j in range(size):
            outs[d][j] = out[d * 128 : (d + 1) * 128, j * 128 : (j + 1) * 128]


def y_transform(size, lead, sides, tab, operands):
    whole = jax.ShapeDtypeStruct((N, size * 128), F32)
    shapes = [whole] if 1 not in sides else [jax.ShapeDtypeStruct((size, 128, 128), F32)] * 4
    return pl.pallas_call(
        functools.partial(y_kernel, size, lead, sides),
        out_shape=shapes,
        in_specs=[VM] * (1 + len(operands)),
        out_specs=[VM] * len(shapes),
        scratch_shapes=[pltpu.VMEM((2, 256 * len(sides), size * 128), BF)],
        compiler_params=params(12),
        cost_estimate=pl.CostEstimate(
            flops=3 * len(sides) * size * N * N * 128, bytes_accessed=2**20 + size * 2**19, transcendentals=0
        ),
        name="y_transform",
    )(tab, *operands)


def z_right(tab, shifts):
    here = lax.axis_index("zb")
    order = [(here + 4 - d) % 4 * 128 for d in shifts]
    return jnp.concatenate(
        [tab[pl.ds(pl.multiple_of(part * N + o, 128), 128), :] for part in (0, 1, 0) for o in order]
    )


def z_dot(fields, rows, right):
    field = jnp.concatenate([jnp.concatenate([f[j] for f in fields], axis=1) for j in rows])
    high, low = halves(field)
    left = jnp.concatenate([high, high, low], axis=1)
    return jnp.dot(left, right, preferred_element_type=F32)


def z_part_kernel(size, shifts, tab, *refs):
    fields, out = refs[:-1], refs[-1]
    right = z_right(tab, shifts)
    for rows in (range(size // 2), range(size // 2, size)):
        value = z_dot(fields, rows, right)
        for i, j in enumerate(rows):
            out[j] = value[i * 128 : (i + 1) * 128]


def z_part(size, shifts, tab, fields):
    return pl.pallas_call(
        functools.partial(z_part_kernel, size, shifts),
        out_shape=jax.ShapeDtypeStruct((size, 128, N), F32),
        in_specs=[VM] * (1 + len(fields)),
        out_specs=VM,
        compiler_params=params(12),
        cost_estimate=pl.CostEstimate(
            flops=3 * size * 128 * N * N, bytes_accessed=2**20 + size * 2**19, transcendentals=0
        ),
        name="z_part",
    )(tab, *fields)


def z_scale_kernel(start, size, sx, sy, sz, out):
    yz = y_plus_z(sy, sz)
    base = lax.axis_index("ya") * 16 + start
    for j in range(size):
        out[j] = lax.rsqrt(sx[base + j] + yz)


def y_plus_z(sy, sz):
    at = pl.multiple_of(lax.axis_index("zb") * 128, 128)
    along = jnp.broadcast_to(sy[:, pl.ds(at, 128)], (128, 128)).T
    return jnp.concatenate([along] * 4, axis=1) + sz[...]


def z_scale(start, size, sx, sy, sz):
    return pl.pallas_call(
        functools.partial(z_scale_kernel, start, size),
        out_shape=jax.ShapeDtypeStruct((size, 128, N), F32),
        in_specs=[pl.BlockSpec(memory_space=pltpu.SMEM), VM, VM],
        out_specs=VM,
        compiler_params=params(2),
        cost_estimate=pl.CostEstimate(
            flops=size * 128 * N * 4, bytes_accessed=size * 2**18, transcendentals=size * 128 * N
        ),
        name="z_scale",
    )(sx, sy, sz)


def z_kernel(start, size, shifts, partial, pieces, tab, *refs):
    out, result, sem = refs[-3:]
    right = z_right(tab, shifts)
    if partial:
        scale, before, fields = refs[0], refs[1], refs[2:]
    else:
        sx, fields = refs[0], refs[3:]
        yz = y_plus_z(*refs[1:3])
        base = lax.axis_index("ya") * 16 + start
    copies = []
    cuts = [size * n // pieces for n in range(pieces + 1)]
    for begin, end in zip(cuts, cuts[1:]):
        value = z_dot(fields[: len(shifts)], range(begin, end), right)
        for j in range(begin, end):
            part = value[(j - begin) * 128 : (j - begin + 1) * 128]
            if partial:
                result[j] = (part + before[j]) * scale[j]
            else:
                result[j] = part * lax.rsqrt(sx[base + j] + yz)
            copy = pltpu.make_async_copy(result.at[j], out.at[start + j], sem.at[j])
            copy.start()
            copies.append(copy)
    for copy in copies:
        copy.wait()


def z_transform(start, size, shifts, partial, tab, more, fields, into):
    back = [] if into is None else [into]
    count = len(more) + len(fields)
    specs = [VM] * (1 + count) + [pl.BlockSpec(memory_space=pltpu.HBM)] * len(back)
    if not partial:
        specs[1] = pl.BlockSpec(memory_space=pltpu.SMEM)
    return pl.pallas_call(
        functools.partial(z_kernel, start, size, shifts, partial, 3 if partial else 2),
        out_shape=jax.ShapeDtypeStruct((16, 128, N), F32),
        in_specs=specs,
        out_specs=pl.BlockSpec(memory_space=pltpu.HBM),
        scratch_shapes=[pltpu.VMEM((size, 128, N), F32), pltpu.SemaphoreType.DMA((size,))],
        input_output_aliases={1 + count: 0} if back else {},
        compiler_params=params(12),
        cost_estimate=pl.CostEstimate(
            flops=6 * size * 128 * N * N, bytes_accessed=2**20 + size * 2**19, transcendentals=size * 128 * N
        ),
        name="z_transform",
    )(tab, *more, *fields, *back)


SHIFTS = (1, 3, 2)


def run(source, symbol_x, symbol_y, symbol_z):
    h = table()
    high = h.astype(jnp.bfloat16)
    low = (h - high.astype(np.float32)).astype(jnp.bfloat16)
    y_tab = np.stack([high, low], axis=1).reshape(N, 2, 16, 2, 16).transpose(0, 1, 3, 2, 4)
    y_tab = jnp.asarray(y_tab.reshape(N, 2 * N))
    z_tab = jnp.asarray(np.concatenate([high, low]))

    sy, sz = symbol_y[None, :], symbol_z[None, :]

    swap = [(a, a ^ 1) for a in range(32)]
    made = []
    for k, size in enumerate(CHUNKS):
        outs = x_transform(source if k == 0 else field, STARTS[k], size, LEADS[k], k == 0)
        made.append(outs[:4])
        field = outs[4] if k == 0 else field
    out, arrived = None, None
    for k, size in enumerate(CHUNKS):
        if arrived is None:
            b, skip = {}, 0
            for d in SHIFTS:
                b[d] = lax.ppermute(made[k][d], "ya", ring_pairs(LEADS[k], d))
        else:
            b, skip = arrived, CHUNKS[k - 1] * 128
        merge = k in MERGED
        after = made[k + 1][1:] if merge else []
        groups = regroup(size, skip, [made[k][0], b[1], b[2], b[3]], after)
        c = {}
        for d in SHIFTS:
            c[d] = lax.ppermute(groups[d], "ya", ring_pairs(1 - LEADS[k], d))
        arrived = c if merge else None
        c = [groups[0], c[1], c[2], c[3]]
        other = gather_other(size, c)
        other = lax.ppermute(other, "ya", swap)
        if k == 0:
            early = y_transform(size, LEADS[k], (0,), y_tab, c)[0]
            f = y_transform(size, LEADS[k], (1,), y_tab, [other, early])
        else:
            f = y_transform(size, LEADS[k], (0, 1), y_tab, [*c, other])
        g = {0: f[0]}
        for d in SHIFTS:
            pairs = [(n, (n + d) % 4) for n in range(4)]
            g[d] = lax.ppermute(f[d], "zb", pairs)
        shifts, more, last = (0, *SHIFTS), [symbol_x, sy, sz], k == len(CHUNKS) - 1
        if last:
            shifts, early = shifts[3:], shifts[:3]
            more = [z_scale(STARTS[k], size, symbol_x, sy, sz)]
            more.append(z_part(size, early, z_tab, [g[d] for d in early]))
        fields = [g[d] for d in shifts]
        out = z_transform(STARTS[k], size, shifts, last, z_tab, more, fields, out)
    return out


def solution(mesh):
    placed = (P(None, "ya", "zb"), P(), P(), P())
    return jax.shard_map(
        run, mesh=mesh, in_specs=placed, out_specs=P("ya", "zb", None), check_vma=False
    )
```
